32 devices in a mesh: layer: 2 (over x), row: 4 (over z), col: 4 (over y, core).
Axes of the slice: x: 2, y: 2, z: 4, core: 2. Of those that a mesh axis runs over, the one named last changes fastest.
Arguments:
- left_matrix: float32 [2, 1024, 16384], P(None, 'row', 'col'), may hold values from -6 to 6
- right_matrix: float32 [2, 16384, 512], P(None, 'row', 'col'), may hold values from -0.03125 to 0.03125
Outputs:
- product: float32 [2, 1024, 512], P(None, 'row', 'col')
The draws below stay inside these ranges and needn't reach their ends.
All inputs are finite; a program needn't handle non-finite values.
Results may differ from the reference program's by a relative error of at most 0.000071.
Values sent between devices are 32-bit elements; how exact they have to be, the bound alone decides.
A program may use at most 128 MiB of HBM per device.

```python
import jax
import jax.numpy as jnp
from jax import lax

K = 16384
M = 1024
NC = 512


def block_scale(key, dims, cuts, smallest, largest):
    gain, own = 1.0, jax.random.fold_in(key, 6)
    for axis_at, shards_of in cuts:
        draws = jnp.exp(jax.random.uniform(jax.random.fold_in(own, axis_at), (shards_of,), jnp.float32, smallest / len(cuts), largest / len(cuts)))
        gain = gain * jnp.repeat(draws, dims[axis_at] // shards_of).reshape([-1 if axis == axis_at else 1 for axis in range(len(dims))])
    return gain


def gaussian(own_key, dims, width, most, cuts=(), kind=jnp.bfloat16):
    entries = width * jax.random.normal(own_key, dims, jnp.float32)
    if cuts:
        entries = entries * block_scale(own_key, dims, cuts, -0.22, 0.18)
    return jnp.clip(entries, -most, most).astype(kind)


def setup_inputs(seed: int = 0) -> dict:
    splits = jax.random.split(jax.random.key(seed), 3)
    left_matrix = gaussian(splits[0], (2, M, K), 1.0, 6.0, ((1, 4), (2, 4)), jnp.float32)
    right_matrix = gaussian(splits[1], (2, K, NC), (2 * K) ** -0.5, 0.03125, ((1, 4), (2, 4)), jnp.float32)
    return dict(left_matrix=left_matrix, right_matrix=right_matrix)


def reference(left_matrix, right_matrix):
    highest = lax.Precision.HIGHEST
    left_real = left_matrix[0]
    left_imag = left_matrix[1]
    right_real = right_matrix[0]
    right_imag = right_matrix[1]
    first_term = jnp.dot(left_real, right_real, precision=highest, preferred_element_type=jnp.float32)
    second_term = jnp.dot(left_imag, right_imag, precision=highest, preferred_element_type=jnp.float32)
    third_term = jnp.dot(left_real + left_imag, right_real + right_imag, precision=highest, preferred_element_type=jnp.float32)
    return jnp.stack([first_term - second_term, third_term - first_term - second_term])
```

```python
import functools

import jax
import jax.numpy as jnp
from jax import lax
from jax.experimental import pallas as pl
from jax.experimental.pallas import tpu as pltpu
from jax.sharding import PartitionSpec as P

CHUNKS = 8
MESH = pl.DeviceIdType.MESH


def kernel(rows, left, right, out, abuf, bbuf, xbuf, acc, xacc, xout, xin, pout, pin, qout, qin,
           own_sem, bsend, rsend, brecv, ysend, yrecv, xsend, xrecv, csend, crecv, psem, qsem):
    x = lax.axis_index("layer")
    z = lax.axis_index("row")
    col = lax.axis_index("col")
    y = col // 2
    c = col % 2
    height = left.shape[1]
    width = right.shape[2]
    share = abuf.shape[3]
    step = share // CHUNKS
    last = rows - 1
    base = x * share
    parity = z % 2
    at_low, at_high = z == 0, z == last
    at_end = at_low | at_high
    lends = (at_low & (c == 1)) | (at_high & (c == 0))
    helps = ((z == 1) & (c == 1)) | ((z == last - 1) & (c == 0))
    inward = jnp.where(at_low, 1, last - 1)
    outward = jnp.where(z == 1, 0, last)
    lent_slot = jnp.where(at_low, 0, (last - 1) // 2)
    lends_own = lends & (y == lent_slot)
    lends_relayed = lends & (y != lent_slot)

    def other(**where):
        return dict(device_id=where, device_id_type=MESH)

    partner = dict(col=y * 2 + 1 - c)
    across = dict(col=(1 - y) * 2 + c)
    copy_x = dict(layer=1 - x)

    barrier = pltpu.get_barrier_semaphore()
    for where in (partner, across, copy_x):
        pl.semaphore_signal(barrier, inc=1, **other(**where))

    @pl.when(z > 0)
    def _():
        for core in range(2):
            pl.semaphore_signal(barrier, inc=1, **other(row=z - 1, col=y * 2 + core))

    @pl.when(z < last)
    def _():
        for core in range(2):
            pl.semaphore_signal(barrier, inc=1, **other(row=z + 1, col=y * 2 + core))

    own_copy = pltpu.make_async_copy(left.at[:, :, pl.ds(base, share)], abuf.at[y], own_sem)
    own_copy.start()
    acc[...] = jnp.zeros_like(acc)
    xacc[...] = jnp.zeros_like(xacc)
    pl.semaphore_wait(barrier, 3 + 2 * ((z > 0).astype(jnp.int32) + (z < last).astype(jnp.int32)))

    def span(i):
        return pl.ds(pl.multiple_of(i * step, step), step)

    def source_span(i):
        return pl.ds(pl.multiple_of(base + i * step, step), step)

    def half(h):
        return pl.ds(pl.multiple_of(h * width, width), width)

    def b_copy(i, way, row):
        return pltpu.make_async_remote_copy(
            src_ref=right.at[:, source_span(i), :],
            dst_ref=bbuf.at[z // 2, :, span(i), half(c)],
            send_sem=bsend.at[way, i], recv_sem=brecv.at[z // 2, c, i],
            **other(row=row, col=y * 2 + parity))

    def b_local(i):
        return pltpu.make_async_copy(
            right.at[:, source_span(i), :], bbuf.at[z // 2, :, span(i), half(c)],
            brecv.at[z // 2, c, i])

    def y_copy(i):
        return pltpu.make_async_remote_copy(
            src_ref=left.at[:, :, source_span(i)], dst_ref=abuf.at[y, :, :, span(i)],
            send_sem=ysend.at[i], recv_sem=yrecv.at[i], **other(**across))

    def y_arrival(i):
        return pltpu.make_async_remote_copy(
            src_ref=left.at[:, :, source_span(i)], dst_ref=abuf.at[1 - y, :, :, span(i)],
            send_sem=ysend.at[i], recv_sem=yrecv.at[i], **other(**across))

    def x_own(i):
        return pltpu.make_async_remote_copy(
            src_ref=left.at[:, :, source_span(i)], dst_ref=xbuf.at[:, :, span(i)],
            send_sem=xsend.at[i], recv_sem=xrecv.at[i], **other(row=inward))

    def x_relay(i):
        return pltpu.make_async_remote_copy(
            src_ref=abuf.at[1 - y, :, :, span(i)], dst_ref=xbuf.at[:, :, span(i)],
            send_sem=xsend.at[i], recv_sem=xrecv.at[i], **other(row=inward))

    sends_up = (z < last) & (z != last - 1)
    sends_down = (z > 0) & (z != 1)

    def launch(i, carry):
        @pl.when(sends_up)
        def _():
            b_copy(i, 0, z + 1).start()

        @pl.when(sends_down)
        def _():
            b_copy(i, 1, z - 1).start()

        y_copy(i).start()

        @pl.when(c == parity)
        def _():
            b_local(i).start()

        @pl.when(c != parity)
        def _():
            b_copy(i, 2, z).start()

        return carry

    lax.fori_loop(0, CHUNKS, launch, 0)

    @pl.when(lends_own)
    def _():
        def lend(i, carry):
            x_own(i).start()
            return carry
        lax.fori_loop(0, CHUNKS, lend, 0)

    own_copy.wait()

    def b_arrival(s, h, i):
        ref = bbuf.at[s, :, span(i), half(h)]
        return pltpu.make_async_copy(ref, ref, brecv.at[s, h, i])

    def relay(s, h, i, row):
        ref = bbuf.at[s, :, span(i), half(h)]
        return pltpu.make_async_remote_copy(
            src_ref=ref, dst_ref=ref, send_sem=rsend.at[s, h, i], recv_sem=brecv.at[s, h, i],
            **other(row=row))

    def present(s):
        quarter = 2 * s + c
        return jnp.logical_not((at_low & (quarter == 1)) | (at_high & (quarter == last - 1)))

    def goes_up(s):
        quarter = 2 * s + c
        return (quarter < z) & (z < last)

    def goes_down(s):
        quarter = 2 * s + c
        return (quarter > z) & (z > 0)

    def multiply(totals, a_ref, s, i):
        a_re, a_im = a_ref[0, :, span(i)], a_ref[1, :, span(i)]
        b_re, b_im = bbuf[s, 0, span(i), :], bbuf[s, 1, span(i), :]
        dot = functools.partial(
            jnp.dot, precision=lax.Precision.HIGHEST, preferred_element_type=jnp.float32)
        totals[0] += dot(a_re, b_re)
        totals[1] += dot(a_im, b_im)
        totals[2] += dot(a_re + a_im, b_re + b_im)

    def right_step(i):
        for s in range(2):
            @pl.when(present(s))
            def _():
                for h in range(2):
                    b_arrival(s, h, i).wait()

                    @pl.when(goes_up(s))
                    def _():
                        relay(s, h, i, z + 1).start()

                    @pl.when(goes_down(s))
                    def _():
                        relay(s, h, i, z - 1).start()

        @pl.when(present(y))
        def _():
            multiply(acc, abuf.at[y], y, i)

    def left_step(i):
        y_arrival(i).wait_recv()

        @pl.when(lends_relayed)
        def _():
            x_relay(i).start()

        @pl.when(present(1 - y))
        def _():
            multiply(acc, abuf.at[1 - y], 1 - y, i)

        @pl.when(helps)
        def _():
            x_own(i).wait_recv()
            multiply(xacc, xbuf, z // 2, i)

    early = jnp.logical_not(at_end) & (c != parity)

    def work(t, carry):
        first = t < CHUNKS
        apart = jnp.where(first, t, t - CHUNKS)
        i = jnp.where(early | lends_relayed, apart, t // 2)
        is_left = ((early & jnp.logical_not(first)) | (lends_relayed & first)
                   | (jnp.logical_not(early | lends_relayed) & (t % 2 == 1)))

        @pl.when(is_left)
        def _():
            left_step(i)

        @pl.when(jnp.logical_not(is_left))
        def _():
            right_step(i)

        return carry

    lax.fori_loop(0, 2 * CHUNKS, work, 0)

    def combined(totals, h):
        first, second, third = (totals[k, :, half(h)] for k in range(3))
        return first - second, third - first - second

    def lend_back(h):
        return pltpu.make_async_remote_copy(
            src_ref=xout.at[h], dst_ref=xin, send_sem=csend.at[h], recv_sem=crecv,
            **other(row=outward, col=y * 2 + h))

    @pl.when(helps)
    def _():
        for h in range(2):
            xout[h, 0], xout[h, 1] = combined(xacc, h)
        for h in range(2):
            lend_back(h).start()

    pout[0], pout[1] = combined(acc, 1 - c)
    to_partner = pltpu.make_async_remote_copy(
        src_ref=pout, dst_ref=pin, send_sem=psem.at[0], recv_sem=psem.at[1], **other(**partner))
    to_partner.start()
    mine_re, mine_im = combined(acc, c)
    qout[0] = mine_re
    qout[1] = mine_im
    to_partner.wait_recv()
    qout[...] += pin[...]

    @pl.when(at_end)
    def _():
        pltpu.make_async_copy(xin, xin, crecv).wait()
        qout[...] += xin[...]

    to_copy = pltpu.make_async_remote_copy(
        src_ref=qout, dst_ref=qin, send_sem=qsem.at[0], recv_sem=qsem.at[1], **other(**copy_x))
    to_copy.start()

    def settle(i, carry):
        @pl.when(sends_up)
        def _():
            b_copy(i, 0, z).wait_send()

        @pl.when(sends_down)
        def _():
            b_copy(i, 1, z).wait_send()

        @pl.when(c != parity)
        def _():
            b_copy(i, 2, z).wait_send()

        y_copy(i).wait_send()

        @pl.when(lends)
        def _():
            x_own(i).wait_send()

        for s in range(2):
            @pl.when(present(s) & (goes_up(s) | goes_down(s)))
            def _():
                for h in range(2):
                    relay(s, h, i, z).wait_send()

        return carry

    lax.fori_loop(0, CHUNKS, settle, 0)

    @pl.when(helps)
    def _():
        for h in range(2):
            lend_back(h).wait_send()

    to_partner.wait_send()
    to_copy.wait()
    out[...] = qout[...] + qin[...]


def lent_product(left_matrix, right_matrix, layers, rows):
    height = left_matrix.shape[1]
    width = right_matrix.shape[2]
    share = left_matrix.shape[2] // layers
    f32 = jnp.float32
    dma = pltpu.SemaphoreType.DMA
    block = (2, height, width)
    return pl.pallas_call(
        functools.partial(kernel, rows),
        out_shape=jax.ShapeDtypeStruct(block, f32),
        in_specs=[pl.BlockSpec(memory_space=pl.ANY)] * 2,
        out_specs=pl.BlockSpec(memory_space=pltpu.VMEM),
        scratch_shapes=[
            pltpu.VMEM((2, 2, height, share), f32),
            pltpu.VMEM((2, 2, share, 2 * width), f32),
            pltpu.VMEM((2, height, share), f32),
            pltpu.VMEM((3, height, 2 * width), f32),
            pltpu.VMEM((3, height, 2 * width), f32),
            pltpu.VMEM((2,) + block, f32),
            pltpu.VMEM(block, f32),
            pltpu.VMEM(block, f32),
            pltpu.VMEM(block, f32),
            pltpu.VMEM(block, f32),
            pltpu.VMEM(block, f32),
            dma,
            dma((3, CHUNKS)),
            dma((2, 2, CHUNKS)),
            dma((2, 2, CHUNKS)),
            dma((CHUNKS,)),
            dma((CHUNKS,)),
            dma((CHUNKS,)),
            dma((CHUNKS,)),
            dma((2,)),
            dma,
            dma((2,)),
            dma((2,)),
        ],
        compiler_params=pltpu.CompilerParams(
            collective_id=0, has_side_effects=True, vmem_limit_bytes=60 * 2**20),
    )(left_matrix, right_matrix)


def gathered_product(left_matrix, right_matrix, layers):
    layer_index = lax.axis_index("layer")
    local_cols = right_matrix.shape[2]
    left_width = left_matrix.shape[2]
    right_height = right_matrix.shape[1]
    share_width = left_width // layers
    group_count = right_height // left_width
    left_own = lax.dynamic_slice_in_dim(left_matrix, layer_index * share_width, share_width, 2)
    right_view = right_matrix.reshape(2, group_count, layers, share_width, local_cols)
    right_own = lax.dynamic_slice_in_dim(right_view, layer_index, 1, 2)
    right_own = right_own.reshape(2, group_count * share_width, local_cols)
    right_whole = lax.all_gather(right_own, "row", axis=1, tiled=True)
    left_whole = lax.all_gather(left_own, "col", axis=2, tiled=True)
    dot = functools.partial(
        jnp.dot, precision=lax.Precision.HIGHEST, preferred_element_type=jnp.float32)
    first_term = dot(left_whole[0], right_whole[0])
    second_term = dot(left_whole[1], right_whole[1])
    third_term = dot(left_whole[0] + left_whole[1], right_whole[0] + right_whole[1])
    partial_product = jnp.stack([first_term - second_term, third_term - first_term - second_term])
    return lax.psum(partial_product, "layer")


def local(left_matrix, right_matrix):
    layers = lax.axis_size("layer")
    rows = lax.axis_size("row")
    cols = lax.axis_size("col")
    if layers == 2 and rows == cols == 4:
        return lent_product(left_matrix, right_matrix, layers, rows)
    return gathered_product(left_matrix, right_matrix, layers)


def solution(mesh):
    in_specs = (P(None, "row", "col"), P(None, "row", "col"))
    out_specs = P(None, "row", "col")
    return jax.shard_map(local, mesh=mesh, in_specs=in_specs, out_specs=out_specs, check_vma=False)
```

```python
import functools

import jax
import jax.numpy as jnp
from jax import lax
from jax.experimental import pallas as pl
from jax.experimental.pallas import tpu as pltpu
from jax.sharding import PartitionSpec as P

CHUNKS = 16
MESH = pl.DeviceIdType.MESH


def kernel(rows, left, right, out, abuf, bbuf, xbuf, acc, xacc, xout, xin, pout, pin, qout, qin,
           own_sem, bsend, rsend, brecv, ysend, yrecv, xsend, xrecv, csend, crecv, psem, qsem, turn):
    x = lax.axis_index("layer")
    z = lax.axis_index("row")
    col = lax.axis_index("col")
    y = col // 2
    c = col % 2
    height = left.shape[1]
    width = right.shape[2]
    share = abuf.shape[3]
    step = share // CHUNKS
    last = rows - 1
    base = x * share
    parity = z % 2
    at_low, at_high = z == 0, z == last
    at_end = at_low | at_high
    lends = (at_low & (c == 1)) | (at_high & (c == 0))
    helps = ((z == 1) & (c == 1)) | ((z == last - 1) & (c == 0))
    inward = jnp.where(at_low, 1, last - 1)
    outward = jnp.where(z == 1, 0, last)
    lent_slot = jnp.where(at_low, 0, (last - 1) // 2)
    lends_own = lends & (y == lent_slot)
    lends_relayed = lends & (y != lent_slot)

    def other(**where):
        return dict(device_id=where, device_id_type=MESH)

    partner = dict(col=y * 2 + 1 - c)
    across = dict(col=(1 - y) * 2 + c)
    copy_x = dict(layer=1 - x)

    barrier = pltpu.get_barrier_semaphore()
    for where in (partner, across, copy_x):
        pl.semaphore_signal(barrier, inc=1, **other(**where))

    @pl.when(z > 0)
    def _():
        for core in range(2):
            pl.semaphore_signal(barrier, inc=1, **other(row=z - 1, col=y * 2 + core))

    @pl.when(z < last)
    def _():
        for core in range(2):
            pl.semaphore_signal(barrier, inc=1, **other(row=z + 1, col=y * 2 + core))

    own_copy = pltpu.make_async_copy(left.at[:, :, pl.ds(base, share)], abuf.at[y], own_sem)
    own_copy.start()
    acc[...] = jnp.zeros_like(acc)
    xacc[...] = jnp.zeros_like(xacc)
    pl.semaphore_wait(barrier, 3 + 2 * ((z > 0).astype(jnp.int32) + (z < last).astype(jnp.int32)))

    def span(i):
        return pl.ds(pl.multiple_of(i * step, step), step)

    def source_span(i):
        return pl.ds(pl.multiple_of(base + i * step, step), step)

    def half(h):
        return pl.ds(pl.multiple_of(h * width, width), width)

    def b_copy(i, way, row):
        return pltpu.make_async_remote_copy(
            src_ref=right.at[:, source_span(i), :],
            dst_ref=bbuf.at[z // 2, c, :, span(i), :],
            send_sem=bsend.at[way, i], recv_sem=brecv.at[z // 2, c, i],
            **other(row=row, col=y * 2 + parity))

    def b_local(i):
        return pltpu.make_async_copy(
            right.at[:, source_span(i), :], bbuf.at[z // 2, c, :, span(i), :],
            brecv.at[z // 2, c, i])

    def y_copy(i):
        return pltpu.make_async_remote_copy(
            src_ref=left.at[:, :, source_span(i)], dst_ref=abuf.at[y, :, :, span(i)],
            send_sem=ysend.at[i], recv_sem=yrecv.at[i], **other(**across))

    def y_arrival(i):
        return pltpu.make_async_remote_copy(
            src_ref=left.at[:, :, source_span(i)], dst_ref=abuf.at[1 - y, :, :, span(i)],
            send_sem=ysend.at[i], recv_sem=yrecv.at[i], **other(**across))

    def x_own(i):
        return pltpu.make_async_remote_copy(
            src_ref=left.at[:, :, source_span(i)], dst_ref=xbuf.at[:, :, span(i)],
            send_sem=xsend.at[i], recv_sem=xrecv.at[i], **other(row=inward))

    def x_relay(i):
        return pltpu.make_async_remote_copy(
            src_ref=abuf.at[1 - y, :, :, span(i)], dst_ref=xbuf.at[:, :, span(i)],
            send_sem=xsend.at[i], recv_sem=xrecv.at[i], **other(row=inward))

    yields = at_end & jnp.logical_not(lends) & (y == lent_slot)
    sends_up = (z < last) & (z != last - 1)
    sends_down = (z > 0) & (z != 1)

    def launch(i, carry):
        @pl.when(sends_up)
        def _():
            b_copy(i, 0, z + 1).start()

        @pl.when(sends_down)
        def _():
            b_copy(i, 1, z - 1).start()

        @pl.when(jnp.logical_not(yields))
        def _():
            y_copy(i).start()

        @pl.when(c == parity)
        def _():
            b_local(i).start()

        @pl.when(c != parity)
        def _():
            b_copy(i, 2, z).start()

        return carry

    lax.fori_loop(0, CHUNKS, launch, 0)

    @pl.when(lends_own)
    def _():
        def lend(i, carry):
            x_own(i).start()
            return carry
        lax.fori_loop(0, CHUNKS, lend, 0)

    @pl.when(lends_own)
    def _():
        def crossed(i, carry):
            y_copy(i).wait_send()
            return carry
        lax.fori_loop(0, CHUNKS - 1, crossed, 0)
        pl.semaphore_signal(turn, inc=1, **other(**partner))

    @pl.when(yields)
    def _():
        pl.semaphore_wait(turn, 1)

        def cross(i, carry):
            y_copy(i).start()
            return carry
        lax.fori_loop(0, CHUNKS, cross, 0)

    own_copy.wait()

    def b_arrival(s, h, i):
        ref = bbuf.at[s, h, :, span(i), :]
        return pltpu.make_async_copy(ref, ref, brecv.at[s, h, i])

    def relay(s, h, i, row):
        ref = bbuf.at[s, h, :, span(i), :]
        return pltpu.make_async_remote_copy(
            src_ref=ref, dst_ref=ref, send_sem=rsend.at[s, h, i], recv_sem=brecv.at[s, h, i],
            **other(row=row))

    def present(s):
        quarter = 2 * s + c
        return jnp.logical_not((at_low & (quarter == 1)) | (at_high & (quarter == last - 1)))

    def goes_up(s):
        quarter = 2 * s + c
        return (quarter < z) & (z < last)

    def goes_down(s):
        quarter = 2 * s + c
        return (quarter > z) & (z > 0)

    def split(value):
        high = value.astype(jnp.bfloat16)
        return high, (value - high.astype(jnp.float32)).astype(jnp.bfloat16)

    def dot(a, b):
        a_high, a_low = split(a)
        b_high, b_low = split(b)
        return jnp.dot(
            jnp.concatenate([a_high, a_high, a_low], axis=1),
            jnp.concatenate([b_high, b_low, b_high], axis=0),
            preferred_element_type=jnp.float32)

    def multiply(totals, a_ref, s, i):
        @pl.when(i % 2 == 1)
        def _():
            at = pl.ds(pl.multiple_of((i - 1) * step, 2 * step), 2 * step)
            a_re, a_im = a_ref[0, :, at], a_ref[1, :, at]
            b_re, b_im = (
                jnp.concatenate([bbuf[s, h, k, at, :] for h in range(2)], axis=1)
                for k in range(2))
            totals[0] += dot(a_re, b_re)
            totals[1] += dot(a_im, b_im)
            totals[2] += dot(a_re + a_im, b_re + b_im)

    def right_step(i):
        for s in range(2):
            @pl.when(present(s))
            def _():
                for h in range(2):
                    b_arrival(s, h, i).wait()

                    @pl.when(goes_up(s))
                    def _():
                        relay(s, h, i, z + 1).start()

                    @pl.when(goes_down(s))
                    def _():
                        relay(s, h, i, z - 1).start()

        @pl.when(present(y))
        def _():
            multiply(acc, abuf.at[y], y, i)

    def left_step(i):
        y_arrival(i).wait_recv()

        @pl.when(lends_relayed)
        def _():
            x_relay(i).start()

        @pl.when(present(1 - y))
        def _():
            multiply(acc, abuf.at[1 - y], 1 - y, i)

        @pl.when(helps)
        def _():
            x_own(i).wait_recv()
            multiply(xacc, xbuf, z // 2, i)

    early = jnp.logical_not(at_end) & (c != parity)

    def work(t, carry):
        first = t < CHUNKS
        apart = jnp.where(first, t, t - CHUNKS)
        i = jnp.where(early | lends_relayed, apart, t // 2)
        is_left = ((early & jnp.logical_not(first)) | (lends_relayed & first)
                   | (jnp.logical_not(early | lends_relayed) & (t % 2 == 1)))

        @pl.when(is_left)
        def _():
            left_step(i)

        @pl.when(jnp.logical_not(is_left))
        def _():
            right_step(i)

        return carry

    lax.fori_loop(0, 2 * CHUNKS, work, 0)

    def combined(totals, h):
        first, second, third = (totals[k, :, half(h)] for k in range(3))
        return first - second, third - first - second

    def lend_back(h):
        return pltpu.make_async_remote_copy(
            src_ref=xout.at[h], dst_ref=xin, send_sem=csend.at[h], recv_sem=crecv,
            **other(row=outward, col=y * 2 + h))

    @pl.when(helps)
    def _():
        for h in range(2):
            xout[h, 0], xout[h, 1] = combined(xacc, h)
        for h in range(2):
            lend_back(h).start()

    pout[0], pout[1] = combined(acc, 1 - c)
    to_partner = pltpu.make_async_remote_copy(
        src_ref=pout, dst_ref=pin, send_sem=psem.at[0], recv_sem=psem.at[1], **other(**partner))
    to_partner.start()
    mine_re, mine_im = combined(acc, c)
    qout[0] = mine_re
    qout[1] = mine_im
    to_partner.wait_recv()
    qout[...] += pin[...]

    @pl.when(at_end)
    def _():
        pltpu.make_async_copy(xin, xin, crecv).wait()
        qout[...] += xin[...]

    to_copy = pltpu.make_async_remote_copy(
        src_ref=qout, dst_ref=qin, send_sem=qsem.at[0], recv_sem=qsem.at[1], **other(**copy_x))
    to_copy.start()

    def settle(i, carry):
        @pl.when(sends_up)
        def _():
            b_copy(i, 0, z).wait_send()

        @pl.when(sends_down)
        def _():
            b_copy(i, 1, z).wait_send()

        @pl.when(c != parity)
        def _():
            b_copy(i, 2, z).wait_send()

        @pl.when(jnp.logical_not(lends_own & (i < CHUNKS - 1)))
        def _():
            y_copy(i).wait_send()

        @pl.when(lends)
        def _():
            x_own(i).wait_send()

        for s in range(2):
            @pl.when(present(s) & (goes_up(s) | goes_down(s)))
            def _():
                for h in range(2):
                    relay(s, h, i, z).wait_send()

        return carry

    lax.fori_loop(0, CHUNKS, settle, 0)

    @pl.when(helps)
    def _():
        for h in range(2):
            lend_back(h).wait_send()

    to_partner.wait_send()
    to_copy.wait()
    out[...] = qout[...] + qin[...]


def lent_product(left_matrix, right_matrix, layers, rows):
    height = left_matrix.shape[1]
    width = right_matrix.shape[2]
    share = left_matrix.shape[2] // layers
    f32 = jnp.float32
    dma = pltpu.SemaphoreType.DMA
    block = (2, height, width)
    return pl.pallas_call(
        functools.partial(kernel, rows),
        out_shape=jax.ShapeDtypeStruct(block, f32),
        in_specs=[pl.BlockSpec(memory_space=pl.ANY)] * 2,
        out_specs=pl.BlockSpec(memory_space=pltpu.VMEM),
        scratch_shapes=[
            pltpu.VMEM((2, 2, height, share), f32),
            pltpu.VMEM((2, 2, 2, share, width), f32),
            pltpu.VMEM((2, height, share), f32),
            pltpu.VMEM((3, height, 2 * width), f32),
            pltpu.VMEM((3, height, 2 * width), f32),
            pltpu.VMEM((2,) + block, f32),
            pltpu.VMEM(block, f32),
            pltpu.VMEM(block, f32),
            pltpu.VMEM(block, f32),
            pltpu.VMEM(block, f32),
            pltpu.VMEM(block, f32),
            dma,
            dma((3, CHUNKS)),
            dma((2, 2, CHUNKS)),
            dma((2, 2, CHUNKS)),
            dma((CHUNKS,)),
            dma((CHUNKS,)),
            dma((CHUNKS,)),
            dma((CHUNKS,)),
            dma((2,)),
            dma,
            dma((2,)),
            dma((2,)),
            pltpu.SemaphoreType.REGULAR,
        ],
        compiler_params=pltpu.CompilerParams(
            collective_id=0, has_side_effects=True, vmem_limit_bytes=60 * 2**20),
    )(left_matrix, right_matrix)


def gathered_product(left_matrix, right_matrix, layers):
    layer_index = lax.axis_index("layer")
    local_cols = right_matrix.shape[2]
    left_width = left_matrix.shape[2]
    right_height = right_matrix.shape[1]
    share_width = left_width // layers
    group_count = right_height // left_width
    left_own = lax.dynamic_slice_in_dim(left_matrix, layer_index * share_width, share_width, 2)
    right_view = right_matrix.reshape(2, group_count, layers, share_width, local_cols)
    right_own = lax.dynamic_slice_in_dim(right_view, layer_index, 1, 2)
    right_own = right_own.reshape(2, group_count * share_width, local_cols)
    right_whole = lax.all_gather(right_own, "row", axis=1, tiled=True)
    left_whole = lax.all_gather(left_own, "col", axis=2, tiled=True)
    dot = functools.partial(
        jnp.dot, precision=lax.Precision.HIGHEST, preferred_element_type=jnp.float32)
    first_term = dot(left_whole[0], right_whole[0])
    second_term = dot(left_whole[1], right_whole[1])
    third_term = dot(left_whole[0] + left_whole[1], right_whole[0] + right_whole[1])
    partial_product = jnp.stack([first_term - second_term, third_term - first_term - second_term])
    return lax.psum(partial_product, "layer")


def local(left_matrix, right_matrix):
    layers = lax.axis_size("layer")
    rows = lax.axis_size("row")
    cols = lax.axis_size("col")
    if layers == 2 and rows == cols == 4:
        return lent_product(left_matrix, right_matrix, layers, rows)
    return gathered_product(left_matrix, right_matrix, layers)


def solution(mesh):
    in_specs = (P(None, "row", "col"), P(None, "row", "col"))
    out_specs = P(None, "row", "col")
    return jax.shard_map(local, mesh=mesh, in_specs=in_specs, out_specs=out_specs, check_vma=False)
```
